32 devices in a mesh: path: 8 (over z, core), tm: 4 (over y, x).
Axes of the slice: x: 2, y: 2, z: 4, core: 2. Of those that a mesh axis runs over, the one named last changes fastest.
Arguments:
- shock_rate: float32 [64, 131072], P('tm', 'path'), may hold values from -6 to 6
- shock_fx: float32 [4, 64, 131072], P(None, 'tm', 'path'), may hold values from -6 to 6
- fx_vol: float32 [4], replicated, may hold values from 0.1 to 0.4
- fx_corr: float32 [4], replicated, may hold values from -0.8 to 0.8
- hazard_scale: float32 [32], replicated, may hold values from 0.03 to 3
- counterparty: int32 [512], replicated, may hold values from 0 to 31
- currency: int32 [512], replicated, may hold values from 0 to 3
- maturity: int32 [512], replicated, may hold values from 1 to 64
- notional: float32 [512], replicated, may hold values from -8 to 8
- strike: float32 [512], replicated, may hold values from 0.7 to 1.3
Outputs:
- profile: float32 [64, 32], P('tm')
- cva: float32 [32], replicated
The draws below stay inside these ranges and needn't reach their ends.
All inputs are finite; a program needn't handle non-finite values.
Results may differ from the reference program's by a relative error of at most 0.000061.
Values sent between devices are 32-bit elements; how exact they have to be, the bound alone decides.
A program may use at most 64 MiB of HBM per device.

```python
import math
import jax
import jax.numpy as jnp
from jax import lax

NCCY = 4
NCP = 32
NTRADE = 512
DATES = 64
PATHS = 131072


def plant(drawn, key, least, largest):
    dims = drawn.shape
    place = [jax.random.randint(jax.random.fold_in(key, axis), (), 0, dims[axis]) for axis in range(len(dims))]
    drawn = drawn.at[tuple(place)].set(least)
    longest = dims.index(max(dims))
    place[longest] = (place[longest] + 1) % dims[longest]
    return drawn.at[tuple(place)].set(largest)


def levels(own_key, shape, shards, low, largest):
    factor_of, own = 1.0, jax.random.fold_in(own_key, 6)
    for position, parts in shards:
        steps = jnp.exp(jax.random.uniform(jax.random.fold_in(own, position), (parts,), jnp.float32, low / len(shards), largest / len(shards)))
        factor_of = factor_of * jnp.repeat(steps, shape[position] // parts).reshape([-1 if axis == position else 1 for axis in range(len(shape))])
    return factor_of


def normal_values(stream_key, extent, spread, reach, shards=(), held_as=jnp.bfloat16):
    factor_of = levels(stream_key, extent, shards, -0.22, 0.18) if shards else 1.0
    result = jax.random.normal(stream_key, extent, jnp.float32) * spread * factor_of
    return jnp.minimum(jnp.maximum(result, -reach), reach).astype(held_as)


def setup_inputs(seed: int = 0) -> dict:
    keys = jax.random.split(jax.random.key(seed), 11)
    shock_rate = normal_values(keys[0], (DATES, PATHS), 1.0, 6.0, ((0, 4), (1, 8)), jnp.float32)
    shock_fx = normal_values(keys[1], (NCCY, DATES, PATHS), 1.0, 6.0, ((1, 4), (2, 8)), jnp.float32)
    fx_vol = jnp.clip(jnp.exp(jax.random.uniform(keys[2], (NCCY,), jnp.float32, math.log(0.1), math.log(0.4))), 0.1, 0.4)
    fx_corr = jnp.clip(jax.random.uniform(keys[3], (NCCY,), jnp.float32, -0.8, 0.8), -0.8, 0.8)
    hazard_scale = jnp.clip(jnp.exp(jax.random.uniform(keys[4], (NCP,), jnp.float32, math.log(0.03), math.log(3.0))), 0.03, 3.0)
    counterparty = plant(jax.random.randint(keys[5], (NTRADE,), 0, NCP), jax.random.fold_in(keys[5], 1), 0, NCP - 1).astype(jnp.int32)
    currency = plant(jax.random.randint(keys[6], (NTRADE,), 0, NCCY), jax.random.fold_in(keys[6], 1), 0, NCCY - 1).astype(jnp.int32)
    maturity = plant(jax.random.randint(keys[7], (NTRADE,), 1, DATES + 1), jax.random.fold_in(keys[7], 1), 1, DATES).astype(jnp.int32)
    notional = normal_values(keys[8], (NTRADE,), 2.0, 8.0, (), jnp.float32)
    strike = jnp.clip(jax.random.uniform(keys[9], (NTRADE,), jnp.float32, 0.7, 1.3), 0.7, 1.3)
    return {"shock_rate": shock_rate, "shock_fx": shock_fx, "fx_vol": fx_vol, "fx_corr": fx_corr, "hazard_scale": hazard_scale, "counterparty": counterparty, "currency": currency, "maturity": maturity, "notional": notional, "strike": strike}


HORIZON = 5.0
RATE_DOM = 0.03
RATE_FOR = 0.01
LOSS_SHARE = 0.6
RATE_SHIFT = 1.5
HIGHEST_PREC = lax.Precision.HIGHEST

def trade_tables(date_rows, counterparty, currency, maturity, notional, strike, cp_count, ccy_count, date_step):
    expiry = maturity.astype(jnp.int32)
    is_alive = (date_rows[:, None] < expiry[None, :]).astype(jnp.float32)
    time_left = (expiry[None, :] - date_rows[:, None]).astype(jnp.float32) * date_step
    weight_for = is_alive * notional[None, :] * jnp.exp(-RATE_FOR * time_left)
    weight_dom = is_alive * (notional * strike)[None, :] * jnp.exp(-RATE_DOM * time_left)
    member = (counterparty.astype(jnp.int32)[None, :] == jnp.arange(cp_count, dtype=jnp.int32)[:, None]).astype(jnp.float32)
    currency_onehot = (currency.astype(jnp.int32)[None, :] == jnp.arange(ccy_count, dtype=jnp.int32)[:, None]).astype(jnp.float32)
    fwd_table = jnp.einsum('ck,tk,jk->tcj', member, weight_for, currency_onehot, precision=HIGHEST_PREC)
    dom_table = jnp.einsum('ck,tk->tc', member, weight_dom, precision=HIGHEST_PREC)
    return (fwd_table, dom_table)

def weigh_block(block_item, hazard_scale):
    fwd_table, dom_table, spot, hazard_prev, hazard_cur = block_item
    netted = jnp.einsum('tcj,tjp->tcp', fwd_table, spot, precision=HIGHEST_PREC) - dom_table[:, :, None]
    exposure = jnp.maximum(netted, 0.0)
    scale_row = hazard_scale[None, :, None]
    density = jnp.exp(-scale_row * hazard_prev[:, None, :]) - jnp.exp(-scale_row * hazard_cur[:, None, :])
    return lax.optimization_barrier(jnp.sum(exposure * density, axis=2))

def weigh_dates(fwd_table, dom_table, spot, hazard_prev, hazard_cur, hazard_scale):
    date_count, path_count = hazard_cur.shape
    cp_count = dom_table.shape[1]
    ccy_count = spot.shape[1]
    block_dates = math.gcd(date_count, max(1, 32768 // path_count))
    groups = date_count // block_dates
    blocks = (fwd_table.reshape(groups, block_dates, cp_count, ccy_count), dom_table.reshape(groups, block_dates, cp_count), spot.reshape(groups, block_dates, ccy_count, path_count), hazard_prev.reshape(groups, block_dates, path_count), hazard_cur.reshape(groups, block_dates, path_count))
    weighed = lax.map(lambda block_item: weigh_block(block_item, hazard_scale), blocks)
    return weighed.reshape(date_count, cp_count)

def reference(shock_rate, shock_fx, fx_vol, fx_corr, hazard_scale, counterparty, currency, maturity, notional, strike):
    date_step = HORIZON / DATES
    decay_rate = math.exp(-2.0 / DATES)
    noise_scale = math.sqrt(1.0 - decay_rate * decay_rate)
    mix_weight = jnp.sqrt(1.0 - fx_corr * fx_corr)
    fx_shock = fx_vol * math.sqrt(date_step)
    fx_drift = 0.5 * fx_vol * fx_vol * date_step

    def advance(state, shocks):
        rate_state, hazard, log_spot = state
        rate_shock, other_shock = shocks
        rate_state = decay_rate * rate_state + noise_scale * rate_shock
        shifted = rate_state + RATE_SHIFT
        hazard_next = hazard + date_step * (0.1 + 0.5 * shifted * shifted)
        mixed = fx_corr[:, None] * rate_shock[None, :] + mix_weight[:, None] * other_shock
        log_spot = log_spot + (fx_shock[:, None] * mixed - fx_drift[:, None])
        return ((rate_state, hazard_next, log_spot), (hazard, hazard_next, jnp.exp(log_spot)))
    start = (jnp.zeros((PATHS,), jnp.float32), jnp.zeros((PATHS,), jnp.float32), jnp.zeros((NCCY, PATHS), jnp.float32))
    ignored, outputs = lax.scan(advance, start, (shock_rate, jnp.moveaxis(shock_fx, 1, 0)))
    hazard_prev, hazard_cur, spot = outputs
    date_rows = jnp.arange(DATES, dtype=jnp.int32)
    fwd_table, dom_table = trade_tables(date_rows, counterparty, currency, maturity, notional, strike, NCP, NCCY, date_step)
    weighed = weigh_dates(fwd_table, dom_table, spot, hazard_prev, hazard_cur, hazard_scale)
    profile = weighed / (PATHS * date_step)
    discount = jnp.exp(-RATE_DOM * date_step * (date_rows.astype(jnp.float32) + 1.0))
    cva = LOSS_SHARE * date_step * lax.optimization_barrier(jnp.sum(discount[:, None] * profile, axis=0))
    return (profile, cva)
```

```python
import functools
import math

import jax
import jax.numpy as jnp
from jax import lax
from jax.experimental import pallas as pl
from jax.experimental.pallas import tpu as pltpu
from jax.sharding import PartitionSpec as P

HORIZON = 5.0
RATE_DOM = 0.03
RATE_FOR = 0.01
LOSS_SHARE = 0.6
RATE_SHIFT = 1.5
BASE_INTENSITY = 0.1
LOG2E = math.log2(math.e)
HIGHEST = lax.Precision.HIGHEST
MESH = pl.DeviceIdType.MESH
F32 = jnp.float32
BF16 = jnp.bfloat16

CHUNKS = 8
WALK_BLOCK = 512
MAIN_BLOCK = 256


def iota(shape, dim):
    return lax.broadcasted_iota(jnp.int32, shape, dim)


def halves(x):
    top = x.astype(BF16)
    return top, (x - top.astype(F32)).astype(BF16)


def pick(index, values):
    out = jnp.zeros(index.shape, F32)
    for place, value in values:
        out = jnp.where(index == place, value, out)
    return out


def kernel(
    sizes,
    vol_ref,
    corr_ref,
    scale_ref,
    party_ref,
    ccy_ref,
    mat_ref,
    notional_ref,
    strike_ref,
    rate_hbm,
    fx_hbm,
    profile_ref,
    cva_ref,
    rate_in,
    fx_in,
    walk,
    coef,
    table,
    pay,
    recv,
    state,
    inten,
    acc,
    scale_col,
    bias_col,
    row_out,
    row_recv,
    cva_out,
    cva_recv,
    in_sem,
    send_sem,
    recv_sem,
    row_send_sem,
    row_recv_sem,
    cva_send_sem,
    cva_recv_sem,
):
    dates, paths, nccy, ncp, n_tm, n_path, total_dates, total_paths = sizes
    rounds = n_tm.bit_length() - 1
    chunk = paths // CHUNKS
    dt = HORIZON / total_dates
    lam = 2.0 / total_dates
    decay = math.exp(-lam)
    noise = math.sqrt(1.0 - decay * decay)
    gains = [decay ** (dates << k) for k in range(rounds)]
    quads = [
        0.5 * dt * sum(decay ** (2 * (t + 1)) for t in range(dates << k)) for k in range(rounds)
    ]
    shift = dates.bit_length() - 1
    walk_rows = (nccy + 1) * dates
    fx_rows = nccy * dates

    tm = lax.axis_index("tm")
    me = lax.axis_index("path")
    first_date = tm * dates

    def fetch(c):
        cols = pl.ds(pl.multiple_of(c * chunk, chunk), chunk)
        return (
            pltpu.make_async_copy(rate_hbm.at[:, cols], rate_in.at[:, cols], in_sem.at[0, c]),
            pltpu.make_async_copy(fx_hbm.at[:, :, cols], fx_in.at[:, :, cols], in_sem.at[1, c]),
        )

    for c in range(CHUNKS):
        for copy in fetch(c):
            copy.start()

    barrier = pltpu.get_barrier_semaphore()
    for step in range(1, n_tm):
        other = lax.rem(tm + step, n_tm)
        pl.semaphore_signal(barrier, inc=1, device_id=(me, other), device_id_type=MESH)
    for step in range(1, n_path):
        other = lax.rem(me + step, n_path)
        pl.semaphore_signal(barrier, inc=1, device_id=(other, tm), device_id_type=MESH)

    width = 3 * walk_rows
    shape = (walk_rows + 16, width)
    row = iota(shape, 0)
    col = iota(shape, 1)
    is_walk = row < walk_rows
    blk = jnp.where(is_walk, row >> shift, row - walk_rows)
    day = jnp.where(is_walk, row & (dates - 1), dates - 1)
    base = jnp.where(
        col >= 2 * walk_rows,
        col - 2 * walk_rows,
        jnp.where(col >= walk_rows, col - walk_rows, col),
    )
    src = base >> shift
    src_day = base & (dates - 1)
    vol = pick(blk, [(j + 1, vol_ref[j]) for j in range(nccy)]) * (math.sqrt(dt) * LOG2E)
    corr = pick(blk, [(j + 1, corr_ref[j]) for j in range(nccy)])
    below = src_day <= day
    gap = jnp.maximum(day - src_day, 0).astype(F32)
    back = src_day.astype(F32)
    value = jnp.where(
        src == 0,
        jnp.where(blk == 0, noise * jnp.exp(-lam * gap), vol * corr),
        jnp.where(src == blk, vol * jnp.sqrt(1.0 - corr * corr), 0.0),
    )
    value = jnp.where(below, value, 0.0)
    slope = (dt / noise) * (jnp.exp(-lam * (back + 1.0)) - jnp.exp(-lam * (2 * dates + 1 - back)))
    value = jnp.where(blk == nccy + 1, jnp.where(src == 0, slope, 0.0), value)
    value = jnp.where(blk > nccy + 1, 0.0, value)
    top, low = halves(value)
    coef[...] = jnp.where(col < 2 * walk_rows, top.astype(F32), low.astype(F32)).astype(BF16)

    prow = iota((8, 128), 0)
    slope_row, quad_row = nccy + 1, nccy + 2
    slope_const = RATE_SHIFT * dt * sum(decay ** (t + 1) for t in range(dates))
    const_rows = pick(prow, [(slope_row, slope_const), (quad_row, BASE_INTENSITY * dt * dates)])

    def wide(rows, count):
        return jnp.concatenate([rows] * (count // 128), axis=1) if count > 128 else rows

    def send(k, c):
        partner = tm ^ (1 << k)
        return pltpu.make_async_remote_copy(
            src_ref=pay.at[k, c],
            dst_ref=recv.at[k, c],
            send_sem=send_sem.at[k, c],
            recv_sem=recv_sem.at[k, c],
            device_id=(me, partner),
            device_id_type=MESH,
        )

    def bit(k):
        return (tm >> k) & 1

    last = rounds - 1

    def start_round(k, c):
        if k < last:
            send(k, c).start()
        else:

            @pl.when(bit(k) == 0)
            def _():
                send(k, c).start()

    def wait_round(k, c):
        if k < last:
            send(k, c).wait_recv()
        else:

            @pl.when(bit(k) == 1)
            def _():
                send(k, c).wait_recv()

    def walk_part(c, first):
        at = c * chunk + first
        cols = pl.ds(pl.multiple_of(at, WALK_BLOCK), WALK_BLOCK)
        x = jnp.concatenate(
            [rate_in[:, cols]] + [fx_in[j, :, cols] for j in range(nccy)], axis=0
        )
        top, low = halves(x)
        out = jnp.dot(
            coef[...], jnp.concatenate([top, low, top], axis=0), preferred_element_type=F32
        )
        walk[:, cols] = out[:walk_rows]
        shifted = out[:dates] + RATE_SHIFT
        square = jnp.sum(shifted * shifted, axis=0, keepdims=True) * (0.5 * dt)
        is_quad = wide(prow, WALK_BLOCK) == quad_row
        ends = out[walk_rows : walk_rows + 8] + wide(const_rows, WALK_BLOCK)
        ends = ends + jnp.where(is_quad, square, 0.0)
        pay[0, c, :, pl.ds(pl.multiple_of(first, WALK_BLOCK), WALK_BLOCK)] = ends

    def walk_chunk(c, carry):
        for copy in fetch(c):
            copy.wait()

        def one(b, carry):
            walk_part(c, b * WALK_BLOCK)
            return carry

        lax.fori_loop(0, chunk // WALK_BLOCK, one, 0)

        if rounds:
            start_round(0, c)
        return carry

    if rounds:

        @pl.when(bit(last) == 0)
        def _():
            recv[last] = jnp.zeros(recv.shape[1:], F32)

    pl.semaphore_wait(barrier, n_tm - 1 + n_path - 1)
    lax.fori_loop(0, CHUNKS, walk_chunk, 0)

    party = party_ref[...]
    expiry = mat_ref[...]
    ntrade = party.shape[1]
    member = jnp.where(iota((ncp, ntrade), 0) == party, 1.0, 0.0).astype(F32)
    date = first_date + iota((dates, ntrade), 0)
    alive = date < expiry
    left = (expiry - date).astype(F32) * dt
    w_for = jnp.where(alive, notional_ref[...] * jnp.exp(-RATE_FOR * left), 0.0)
    w_dom = jnp.where(
        alive, -(notional_ref[...] * strike_ref[...]) * jnp.exp(-RATE_DOM * left), 0.0
    )
    by_ccy = [jnp.where(ccy_ref[...] == j, w_for, 0.0) for j in range(nccy)]
    sums = lax.dot_general(
        member,
        jnp.concatenate(by_ccy * 3 + [w_dom] * 3, axis=0),
        (((1,), (1,)), ((), ())),
        precision=HIGHEST,
        preferred_element_type=F32,
    )
    tcol = iota(sums.shape, 1)
    top = sums.astype(BF16).astype(F32)
    low = (sums - top).astype(BF16).astype(F32)
    rest = sums - top - low
    use_low = ((tcol >= 2 * fx_rows) & (tcol < 3 * fx_rows)) | (
        (tcol >= 3 * fx_rows + dates) & (tcol < 3 * fx_rows + 2 * dates)
    )
    use_rest = tcol >= 3 * fx_rows + 2 * dates
    parts = jnp.where(use_rest, rest, jnp.where(use_low, low, top))
    for t in range(dates):
        table[t * ncp : (t + 1) * ncp, :] = jnp.where(
            (tcol & (dates - 1)) == t, parts, 0.0
        ).astype(BF16)

    crow = iota((ncp, 128), 0)
    scale_col[...] = pick(crow, [(c, scale_ref[c]) for c in range(ncp)]) * (-LOG2E)
    brow = iota((fx_rows, 128), 0)
    bvol = pick(brow >> shift, [(j, vol_ref[j]) for j in range(nccy)])
    bday = (first_date + (brow & (dates - 1)) + 1).astype(F32)
    bias_col[...] = (-0.5 * dt * LOG2E) * bvol * bvol * bday
    acc[...] = jnp.zeros_like(acc)

    def join(k, c):
        mine, theirs = pay[k - 1, c], recv[k - 1, c]
        upper_is_mine = bit(k - 1) == 1
        lower = jnp.where(upper_is_mine, theirs, mine)
        upper = jnp.where(upper_is_mine, mine, theirs)
        gain, quad = gains[k - 1], quads[k - 1]
        rows = wide(prow, chunk)
        end = lower[0:1]
        total = lower * jnp.where(rows == 0, gain, 1.0) + upper * jnp.where(
            rows == slope_row, gain, 1.0
        )
        extra = upper[slope_row : slope_row + 1] * end + quad * end * end
        total = total + jnp.where(rows == slope_row, (2.0 * quad * gain) * end, 0.0)
        total = total + jnp.where(rows == quad_row, extra, 0.0)
        pay[k, c] = total

    def absorb(c):
        now = jnp.zeros((8, chunk), F32)
        rows = wide(prow, chunk)
        for k in reversed(range(rounds)):
            other = recv[k, c]
            end = now[0:1]
            extra = other[slope_row : slope_row + 1] * end + quads[k] * end * end
            then = now * jnp.where(rows == 0, gains[k], 1.0) + other
            then = then + jnp.where(rows == quad_row, extra, 0.0)
            now = then if k == last else jnp.where(bit(k) == 1, then, now)
        state[...] = now

    carry_gain = jnp.exp(-lam * (iota((dates, 128), 0).astype(F32) + 1.0))
    ones = jnp.ones((3 * dates, MAIN_BLOCK), BF16)

    def main_part(c, first):
        at = c * chunk + first
        cols = pl.ds(pl.multiple_of(at, MAIN_BLOCK), MAIN_BLOCK)
        own = pl.ds(pl.multiple_of(first, MAIN_BLOCK), MAIN_BLOCK)
        start = state[:, own]
        shifted = walk[:dates, cols] + wide(carry_gain, MAIN_BLOCK) * start[0:1] + RATE_SHIFT
        inten[...] = (BASE_INTENSITY * dt) + (0.5 * dt) * (shifted * shifted)
        spots = []
        for j in range(nccy):
            log = walk[(j + 1) * dates : (j + 2) * dates, cols] + start[j + 1 : j + 2]
            log = log + wide(bias_col[j * dates : (j + 1) * dates], MAIN_BLOCK)
            spots.append(jnp.exp2(log))
        top, low = halves(jnp.concatenate(spots, axis=0))
        netted = jnp.dot(
            table[...],
            jnp.concatenate([top, low, top, ones], axis=0),
            preferred_element_type=F32,
        )
        scales = wide(scale_col[...], MAIN_BLOCK)
        hazard = start[quad_row : quad_row + 1]
        before = jnp.exp2(scales * hazard)
        for t in range(dates):
            hazard = hazard + inten[t : t + 1, :]
            after = jnp.exp2(scales * hazard)
            part = slice(t * ncp, (t + 1) * ncp)
            term = jnp.maximum(netted[part], 0.0) * (before - after)
            total = acc[part]
            for i in range(MAIN_BLOCK // 128):
                total = total + term[:, i * 128 : (i + 1) * 128]
            acc[part] = total
            before = after

    def main_chunk(c, carry):
        for k in range(1, rounds):
            wait_round(k - 1, c)
            if k < last:
                join(k, c)
                start_round(k, c)
            else:

                @pl.when(bit(k) == 0)
                def _():
                    join(k, c)
                    send(k, c).start()

        if rounds:
            wait_round(last, c)
        absorb(c)

        def one(b, carry):
            main_part(c, b * MAIN_BLOCK)
            return carry

        lax.fori_loop(0, chunk // MAIN_BLOCK, one, 0)
        return carry

    lax.fori_loop(0, CHUNKS, main_chunk, 0)

    local = lax.dot_general(
        jnp.ones((8, 128), F32),
        acc[...],
        (((1,), (1,)), ((), ())),
        precision=HIGHEST,
        preferred_element_type=F32,
    )
    row_out[...] = local[0:1]
    row_recv[me] = local[0:1]

    def row_send(step):
        other = lax.rem(me + step, n_path)
        return pltpu.make_async_remote_copy(
            src_ref=row_out,
            dst_ref=row_recv.at[me],
            send_sem=row_send_sem.at[step],
            recv_sem=row_recv_sem.at[step],
            device_id=(other, tm),
            device_id_type=MESH,
        )

    for step in range(1, n_path):
        row_send(step).start()
    for step in range(1, n_path):
        row_send(step).wait_recv()
    total = row_recv[0]
    for i in range(1, n_path):
        total = total + row_recv[i]
    profile = total * (1.0 / (total_paths * dt))
    profile_ref[...] = profile

    lane = iota((1, dates * ncp), 1)
    day = (first_date + lax.div(lane, ncp) + 1).astype(F32)
    weighed = (LOSS_SHARE * dt) * jnp.exp(-RATE_DOM * dt * day) * profile
    folded = weighed[:, :128]
    for i in range(1, dates * ncp // 128):
        folded = folded + weighed[:, i * 128 : (i + 1) * 128]
    cva_out[...] = folded
    cva_recv[tm] = folded

    def cva_send(step):
        other = lax.rem(tm + step, n_tm)
        return pltpu.make_async_remote_copy(
            src_ref=cva_out,
            dst_ref=cva_recv.at[tm],
            send_sem=cva_send_sem.at[step],
            recv_sem=cva_recv_sem.at[step],
            device_id=(me, other),
            device_id_type=MESH,
        )

    for step in range(1, n_tm):
        cva_send(step).start()
    for step in range(1, n_tm):
        cva_send(step).wait_recv()
    total = cva_recv[0]
    for i in range(1, n_tm):
        total = total + cva_recv[i]
    cva = total
    for i in range(1, 128 // ncp):
        cva = cva + pltpu.roll(total, i * ncp, 1)
    cva_ref[...] = cva

    def drain(c, carry):
        for k in range(rounds):
            if k < last:
                send(k, c).wait_send()
            else:

                @pl.when(bit(k) == 0)
                def _():
                    send(k, c).wait_send()

        return carry

    lax.fori_loop(0, CHUNKS, drain, 0)
    for step in range(1, n_path):
        row_send(step).wait_send()
    for step in range(1, n_tm):
        cva_send(step).wait_send()


def per_device(
    shock_rate,
    shock_fx,
    fx_vol,
    fx_corr,
    hazard_scale,
    counterparty,
    currency,
    maturity,
    notional,
    strike,
):
    dates, paths = shock_rate.shape
    nccy = shock_fx.shape[0]
    ncp = hazard_scale.shape[0]
    n_tm = lax.axis_size("tm")
    n_path = lax.axis_size("path")
    rounds = n_tm.bit_length() - 1
    chunk = paths // CHUNKS
    walk_rows = (nccy + 1) * dates
    smem = pl.BlockSpec(memory_space=pltpu.SMEM)
    vmem = pl.BlockSpec(memory_space=pltpu.VMEM)
    hbm = pl.BlockSpec(memory_space=pl.ANY)
    sizes = (dates, paths, nccy, ncp, n_tm, n_path, dates * n_tm, paths * n_path)
    dma = pltpu.SemaphoreType.DMA
    profile, cva = pl.pallas_call(
        functools.partial(kernel, sizes),
        out_shape=(
            jax.ShapeDtypeStruct((1, dates * ncp), F32),
            jax.ShapeDtypeStruct((1, 128), F32),
        ),
        in_specs=[smem] * 3 + [vmem] * 5 + [hbm] * 2,
        out_specs=(vmem, vmem),
        scratch_shapes=[
            pltpu.VMEM((dates, paths), F32),
            pltpu.VMEM((nccy, dates, paths), F32),
            pltpu.VMEM((walk_rows, paths), F32),
            pltpu.VMEM((walk_rows + 16, 3 * walk_rows), BF16),
            pltpu.VMEM((dates * ncp, 3 * walk_rows), BF16),
            pltpu.VMEM((max(rounds, 1), CHUNKS, 8, chunk), F32),
            pltpu.VMEM((max(rounds, 1), CHUNKS, 8, chunk), F32),
            pltpu.VMEM((8, chunk), F32),
            pltpu.VMEM((dates, MAIN_BLOCK), F32),
            pltpu.VMEM((dates * ncp, 128), F32),
            pltpu.VMEM((ncp, 128), F32),
            pltpu.VMEM((nccy * dates, 128), F32),
            pltpu.VMEM((1, dates * ncp), F32),
            pltpu.VMEM((n_path, 1, dates * ncp), F32),
            pltpu.VMEM((1, 128), F32),
            pltpu.VMEM((n_tm, 1, 128), F32),
            dma((2, CHUNKS)),
            dma((max(rounds, 1), CHUNKS)),
            dma((max(rounds, 1), CHUNKS)),
            dma((n_path,)),
            dma((n_path,)),
            dma((n_tm,)),
            dma((n_tm,)),
        ],
        compiler_params=pltpu.CompilerParams(collective_id=0, has_side_effects=True),
    )(
        fx_vol,
        fx_corr,
        hazard_scale,
        counterparty[None],
        currency[None],
        maturity[None],
        notional[None],
        strike[None],
        shock_rate,
        shock_fx,
    )
    return (profile.reshape(dates, ncp), cva[0, :ncp])


def solution(mesh):
    return jax.shard_map(
        per_device,
        mesh=mesh,
        in_specs=(P("tm", "path"), P(None, "tm", "path"), P(), P(), P(), P(), P(), P(), P(), P()),
        out_specs=(P("tm", None), P()),
        check_vma=False,
    )
```

```python
import functools
import math

import jax
import jax.numpy as jnp
from jax import lax
from jax.experimental import pallas as pl
from jax.experimental.pallas import tpu as pltpu
from jax.sharding import PartitionSpec as P

HORIZON = 5.0
RATE_DOM = 0.03
RATE_FOR = 0.01
LOSS_SHARE = 0.6
RATE_SHIFT = 1.5
BASE_INTENSITY = 0.1
LOG2E = math.log2(math.e)
HIGHEST = lax.Precision.HIGHEST
MESH = pl.DeviceIdType.MESH
F32 = jnp.float32
BF16 = jnp.bfloat16

CHUNKS = 8
WALK_BLOCK = 1024
MAIN_BLOCK = 256
UNROLL = 4


def iota(shape, dim):
    return lax.broadcasted_iota(jnp.int32, shape, dim)


def halves(x):
    top = x.astype(BF16)
    return top, (x - top.astype(F32)).astype(BF16)


def pick(index, values):
    out = jnp.zeros(index.shape, F32)
    for place, value in values:
        out = jnp.where(index == place, value, out)
    return out


def kernel(
    sizes,
    vol_ref,
    corr_ref,
    scale_ref,
    party_ref,
    ccy_ref,
    mat_ref,
    notional_ref,
    strike_ref,
    rate_hbm,
    fx_hbm,
    profile_ref,
    cva_ref,
    rate_in,
    fx_in,
    walk,
    coef,
    table,
    pay,
    recv,
    state,
    inten,
    acc,
    scale_col,
    bias_col,
    row_out,
    row_recv,
    cva_out,
    cva_recv,
    in_sem,
    send_sem,
    recv_sem,
    row_send_sem,
    row_recv_sem,
    cva_send_sem,
    cva_recv_sem,
):
    dates, paths, nccy, ncp, n_tm, n_path, total_dates, total_paths = sizes
    rounds = n_tm.bit_length() - 1
    chunk = paths // CHUNKS
    dt = HORIZON / total_dates
    lam = 2.0 / total_dates
    decay = math.exp(-lam)
    noise = math.sqrt(1.0 - decay * decay)
    gains = [decay ** (dates << k) for k in range(rounds)]
    quads = [
        0.5 * dt * sum(decay ** (2 * (t + 1)) for t in range(dates << k)) for k in range(rounds)
    ]
    shift = dates.bit_length() - 1
    walk_rows = (nccy + 1) * dates
    fx_rows = nccy * dates

    tm = lax.axis_index("tm")
    me = lax.axis_index("path")
    first_date = tm * dates

    def fetch(c):
        cols = pl.ds(pl.multiple_of(c * chunk, chunk), chunk)
        return (
            pltpu.make_async_copy(rate_hbm.at[:, cols], rate_in.at[:, cols], in_sem.at[0, c]),
            pltpu.make_async_copy(fx_hbm.at[:, :, cols], fx_in.at[:, :, cols], in_sem.at[1, c]),
        )

    for c in range(CHUNKS):
        for copy in fetch(c):
            copy.start()

    barrier = pltpu.get_barrier_semaphore()
    for step in range(1, n_tm):
        other = lax.rem(tm + step, n_tm)
        pl.semaphore_signal(barrier, inc=1, device_id=(me, other), device_id_type=MESH)
    for step in range(1, n_path):
        other = lax.rem(me + step, n_path)
        pl.semaphore_signal(barrier, inc=1, device_id=(other, tm), device_id_type=MESH)

    width = 3 * walk_rows
    shape = (walk_rows + 16, width)
    row = iota(shape, 0)
    col = iota(shape, 1)
    is_walk = row < walk_rows
    blk = jnp.where(is_walk, row >> shift, row - walk_rows)
    day = jnp.where(is_walk, row & (dates - 1), dates - 1)
    base = jnp.where(
        col >= 2 * walk_rows,
        col - 2 * walk_rows,
        jnp.where(col >= walk_rows, col - walk_rows, col),
    )
    src = base >> shift
    src_day = base & (dates - 1)
    vol = pick(blk, [(j + 1, vol_ref[j]) for j in range(nccy)]) * (math.sqrt(dt) * LOG2E)
    corr = pick(blk, [(j + 1, corr_ref[j]) for j in range(nccy)])
    below = src_day <= day
    gap = jnp.maximum(day - src_day, 0).astype(F32)
    back = src_day.astype(F32)
    value = jnp.where(
        src == 0,
        jnp.where(blk == 0, noise * jnp.exp(-lam * gap), vol * corr),
        jnp.where(src == blk, vol * jnp.sqrt(1.0 - corr * corr), 0.0),
    )
    value = jnp.where(below, value, 0.0)
    slope = (dt / noise) * (jnp.exp(-lam * (back + 1.0)) - jnp.exp(-lam * (2 * dates + 1 - back)))
    value = jnp.where(blk == nccy + 1, jnp.where(src == 0, slope, 0.0), value)
    value = jnp.where(blk > nccy + 1, 0.0, value)
    top, low = halves(value)
    coef[...] = jnp.where(col < 2 * walk_rows, top.astype(F32), low.astype(F32)).astype(BF16)

    prow = iota((8, 128), 0)
    slope_row, quad_row = nccy + 1, nccy + 2
    slope_const = RATE_SHIFT * dt * sum(decay ** (t + 1) for t in range(dates))
    const_rows = pick(prow, [(slope_row, slope_const), (quad_row, BASE_INTENSITY * dt * dates)])

    def wide(rows, count):
        return jnp.concatenate([rows] * (count // 128), axis=1) if count > 128 else rows

    def send(k, c):
        partner = tm ^ (1 << k)
        return pltpu.make_async_remote_copy(
            src_ref=pay.at[k, c],
            dst_ref=recv.at[k, c],
            send_sem=send_sem.at[k, c],
            recv_sem=recv_sem.at[k, c],
            device_id=(me, partner),
            device_id_type=MESH,
        )

    def bit(k):
        return (tm >> k) & 1

    last = rounds - 1

    def start_round(k, c):
        if k < last:
            send(k, c).start()
        else:

            @pl.when(bit(k) == 0)
            def _():
                send(k, c).start()

    def wait_round(k, c):
        if k < last:
            send(k, c).wait_recv()
        else:

            @pl.when(bit(k) == 1)
            def _():
                send(k, c).wait_recv()

    def walk_part(c, first):
        at = c * chunk + first
        cols = pl.ds(pl.multiple_of(at, WALK_BLOCK), WALK_BLOCK)
        x = jnp.concatenate(
            [rate_in[:, cols]] + [fx_in[j, :, cols] for j in range(nccy)], axis=0
        )
        top, low = halves(x)
        out = jnp.dot(
            coef[...], jnp.concatenate([top, low, top], axis=0), preferred_element_type=F32
        )
        walk[:, cols] = out[:walk_rows]
        shifted = out[:dates] + RATE_SHIFT
        square = jnp.sum(shifted * shifted, axis=0, keepdims=True) * (0.5 * dt)
        is_quad = wide(prow, WALK_BLOCK) == quad_row
        ends = out[walk_rows : walk_rows + 8] + wide(const_rows, WALK_BLOCK)
        ends = ends + jnp.where(is_quad, square, 0.0)
        pay[0, c, :, pl.ds(pl.multiple_of(first, WALK_BLOCK), WALK_BLOCK)] = ends

    def walk_chunk(c, carry):
        for copy in fetch(c):
            copy.wait()

        def one(b, carry):
            walk_part(c, b * WALK_BLOCK)
            return carry

        lax.fori_loop(0, chunk // WALK_BLOCK, one, 0)
        return carry

    if rounds:

        @pl.when(bit(last) == 0)
        def _():
            recv[last] = jnp.zeros(recv.shape[1:], F32)

    party = party_ref[...]
    expiry = mat_ref[...]
    ntrade = party.shape[1]
    member = jnp.where(iota((ncp, ntrade), 0) == party, 1.0, 0.0).astype(F32)
    date = first_date + iota((dates, ntrade), 0)
    alive = date < expiry
    left = (expiry - date).astype(F32) * dt
    w_for = jnp.where(alive, notional_ref[...] * jnp.exp(-RATE_FOR * left), 0.0)
    w_dom = jnp.where(
        alive, -(notional_ref[...] * strike_ref[...]) * jnp.exp(-RATE_DOM * left), 0.0
    )
    by_ccy = [jnp.where(ccy_ref[...] == j, w_for, 0.0) for j in range(nccy)]
    sums = lax.dot_general(
        member,
        jnp.concatenate(by_ccy * 3 + [w_dom] * 3, axis=0),
        (((1,), (1,)), ((), ())),
        precision=HIGHEST,
        preferred_element_type=F32,
    )
    tcol = iota(sums.shape, 1)
    top = sums.astype(BF16).astype(F32)
    low = (sums - top).astype(BF16).astype(F32)
    rest = sums - top - low
    use_low = ((tcol >= 2 * fx_rows) & (tcol < 3 * fx_rows)) | (
        (tcol >= 3 * fx_rows + dates) & (tcol < 3 * fx_rows + 2 * dates)
    )
    use_rest = tcol >= 3 * fx_rows + 2 * dates
    parts = jnp.where(use_rest, rest, jnp.where(use_low, low, top))
    for t in range(dates):
        table[t * ncp : (t + 1) * ncp, :] = jnp.where(
            (tcol & (dates - 1)) == t, parts, 0.0
        ).astype(BF16)

    crow = iota((ncp, 128), 0)
    scale_col[...] = pick(crow, [(c, scale_ref[c]) for c in range(ncp)]) * (-LOG2E)
    brow = iota((fx_rows, 128), 0)
    bvol = pick(brow >> shift, [(j, vol_ref[j]) for j in range(nccy)])
    bday = (first_date + (brow & (dates - 1)) + 1).astype(F32)
    bias_col[...] = (-0.5 * dt * LOG2E) * bvol * bvol * bday
    acc[...] = jnp.zeros_like(acc)

    early = CHUNKS // 2
    lax.fori_loop(0, early, walk_chunk, 0)
    pl.semaphore_wait(barrier, n_tm - 1 + n_path - 1)

    def send_early(c, carry):
        start_round(0, c)
        return carry

    def walk_and_send(c, carry):
        walk_chunk(c, carry)
        start_round(0, c)
        return carry

    if rounds:
        lax.fori_loop(0, early, send_early, 0)
        lax.fori_loop(early, CHUNKS, walk_and_send, 0)
    else:
        lax.fori_loop(early, CHUNKS, walk_chunk, 0)


    def join(k, c):
        mine, theirs = pay[k - 1, c], recv[k - 1, c]
        upper_is_mine = bit(k - 1) == 1
        lower = jnp.where(upper_is_mine, theirs, mine)
        upper = jnp.where(upper_is_mine, mine, theirs)
        gain, quad = gains[k - 1], quads[k - 1]
        rows = wide(prow, chunk)
        end = lower[0:1]
        total = lower * jnp.where(rows == 0, gain, 1.0) + upper * jnp.where(
            rows == slope_row, gain, 1.0
        )
        extra = upper[slope_row : slope_row + 1] * end + quad * end * end
        total = total + jnp.where(rows == slope_row, (2.0 * quad * gain) * end, 0.0)
        total = total + jnp.where(rows == quad_row, extra, 0.0)
        pay[k, c] = total

    def absorb(c):
        now = jnp.zeros((8, chunk), F32)
        rows = wide(prow, chunk)
        for k in reversed(range(rounds)):
            other = recv[k, c]
            end = now[0:1]
            extra = other[slope_row : slope_row + 1] * end + quads[k] * end * end
            then = now * jnp.where(rows == 0, gains[k], 1.0) + other
            then = then + jnp.where(rows == quad_row, extra, 0.0)
            now = then if k == last else jnp.where(bit(k) == 1, then, now)
        state[...] = now

    carry_gain = jnp.exp(-lam * (iota((dates, 128), 0).astype(F32) + 1.0))
    ones = jnp.ones((3 * dates, MAIN_BLOCK), BF16)

    def main_part(c, first, u):
        at = c * chunk + first
        cols = pl.ds(pl.multiple_of(at, MAIN_BLOCK), MAIN_BLOCK)
        own = pl.ds(pl.multiple_of(first, MAIN_BLOCK), MAIN_BLOCK)
        start = state[:, own]
        shifted = walk[:dates, cols] + wide(carry_gain, MAIN_BLOCK) * start[0:1] + RATE_SHIFT
        inten[u] = (BASE_INTENSITY * dt) + (0.5 * dt) * (shifted * shifted)
        spots = []
        for j in range(nccy):
            log = walk[(j + 1) * dates : (j + 2) * dates, cols] + start[j + 1 : j + 2]
            log = log + wide(bias_col[j * dates : (j + 1) * dates], MAIN_BLOCK)
            spots.append(jnp.exp2(log))
        top, low = halves(jnp.concatenate(spots, axis=0))
        netted = jnp.dot(
            table[...],
            jnp.concatenate([top, low, top, ones], axis=0),
            preferred_element_type=F32,
        )
        scales = wide(scale_col[...], MAIN_BLOCK)
        hazard = start[quad_row : quad_row + 1]
        before = jnp.exp2(scales * hazard)
        for t in range(dates):
            hazard = hazard + inten[u, t : t + 1, :]
            after = jnp.exp2(scales * hazard)
            part = slice(t * ncp, (t + 1) * ncp)
            term = jnp.maximum(netted[part], 0.0) * (before - after)
            total = acc[part]
            for i in range(MAIN_BLOCK // 128):
                total = total + term[:, i * 128 : (i + 1) * 128]
            acc[part] = total
            before = after

    def main_chunk(c, carry):
        for k in range(1, rounds):
            wait_round(k - 1, c)
            if k < last:
                join(k, c)
                start_round(k, c)
            else:

                @pl.when(bit(k) == 0)
                def _():
                    join(k, c)
                    send(k, c).start()

        if rounds:
            wait_round(last, c)
        absorb(c)

        def one(b, carry):
            for u in range(UNROLL):
                main_part(c, (b * UNROLL + u) * MAIN_BLOCK, u)
            return carry

        lax.fori_loop(0, chunk // (MAIN_BLOCK * UNROLL), one, 0)
        return carry

    lax.fori_loop(0, CHUNKS, main_chunk, 0)

    local = lax.dot_general(
        jnp.ones((8, 128), F32),
        acc[...],
        (((1,), (1,)), ((), ())),
        precision=HIGHEST,
        preferred_element_type=F32,
    )
    row_out[...] = local[0:1]
    row_recv[me] = local[0:1]

    def row_send(step):
        other = lax.rem(me + step, n_path)
        return pltpu.make_async_remote_copy(
            src_ref=row_out,
            dst_ref=row_recv.at[me],
            send_sem=row_send_sem.at[step],
            recv_sem=row_recv_sem.at[step],
            device_id=(other, tm),
            device_id_type=MESH,
        )

    for step in range(1, n_path):
        row_send(step).start()
    for step in range(1, n_path):
        row_send(step).wait_recv()
    total = row_recv[0]
    for i in range(1, n_path):
        total = total + row_recv[i]
    profile = total * (1.0 / (total_paths * dt))
    for t in range(dates):
        profile_ref[t : t + 1, :] = profile[:, t * ncp : (t + 1) * ncp]

    lane = iota((1, dates * ncp), 1)
    day = (first_date + lax.div(lane, ncp) + 1).astype(F32)
    weighed = (LOSS_SHARE * dt) * jnp.exp(-RATE_DOM * dt * day) * profile
    folded = weighed[:, :128]
    for i in range(1, dates * ncp // 128):
        folded = folded + weighed[:, i * 128 : (i + 1) * 128]
    cva_out[...] = folded
    cva_recv[tm] = folded

    def cva_send(step):
        other = lax.rem(tm + step, n_tm)
        return pltpu.make_async_remote_copy(
            src_ref=cva_out,
            dst_ref=cva_recv.at[tm],
            send_sem=cva_send_sem.at[step],
            recv_sem=cva_recv_sem.at[step],
            device_id=(me, other),
            device_id_type=MESH,
        )

    for step in range(1, n_tm):
        cva_send(step).start()
    for step in range(1, n_tm):
        cva_send(step).wait_recv()
    total = cva_recv[0]
    for i in range(1, n_tm):
        total = total + cva_recv[i]
    cva = total
    for i in range(1, 128 // ncp):
        cva = cva + pltpu.roll(total, i * ncp, 1)
    cva_ref[...] = cva[:, :ncp]

    def drain(c, carry):
        for k in range(rounds):
            if k < last:
                send(k, c).wait_send()
            else:

                @pl.when(bit(k) == 0)
                def _():
                    send(k, c).wait_send()

        return carry

    lax.fori_loop(0, CHUNKS, drain, 0)
    for step in range(1, n_path):
        row_send(step).wait_send()
    for step in range(1, n_tm):
        cva_send(step).wait_send()


def per_device(
    shock_rate,
    shock_fx,
    fx_vol,
    fx_corr,
    hazard_scale,
    counterparty,
    currency,
    maturity,
    notional,
    strike,
):
    dates, paths = shock_rate.shape
    nccy = shock_fx.shape[0]
    ncp = hazard_scale.shape[0]
    n_tm = lax.axis_size("tm")
    n_path = lax.axis_size("path")
    rounds = n_tm.bit_length() - 1
    chunk = paths // CHUNKS
    walk_rows = (nccy + 1) * dates
    smem = pl.BlockSpec(memory_space=pltpu.SMEM)
    vmem = pl.BlockSpec(memory_space=pltpu.VMEM)
    hbm = pl.BlockSpec(memory_space=pl.ANY)
    sizes = (dates, paths, nccy, ncp, n_tm, n_path, dates * n_tm, paths * n_path)
    dma = pltpu.SemaphoreType.DMA
    profile, cva = pl.pallas_call(
        functools.partial(kernel, sizes),
        out_shape=(
            jax.ShapeDtypeStruct((dates, ncp), F32),
            jax.ShapeDtypeStruct((1, ncp), F32),
        ),
        in_specs=[smem] * 3 + [vmem] * 5 + [hbm] * 2,
        out_specs=(vmem, vmem),
        scratch_shapes=[
            pltpu.VMEM((dates, paths), F32),
            pltpu.VMEM((nccy, dates, paths), F32),
            pltpu.VMEM((walk_rows, paths), F32),
            pltpu.VMEM((walk_rows + 16, 3 * walk_rows), BF16),
            pltpu.VMEM((dates * ncp, 3 * walk_rows), BF16),
            pltpu.VMEM((max(rounds, 1), CHUNKS, 8, chunk), F32),
            pltpu.VMEM((max(rounds, 1), CHUNKS, 8, chunk), F32),
            pltpu.VMEM((8, chunk), F32),
            pltpu.VMEM((UNROLL, dates, MAIN_BLOCK), F32),
            pltpu.VMEM((dates * ncp, 128), F32),
            pltpu.VMEM((ncp, 128), F32),
            pltpu.VMEM((nccy * dates, 128), F32),
            pltpu.VMEM((1, dates * ncp), F32),
            pltpu.VMEM((n_path, 1, dates * ncp), F32),
            pltpu.VMEM((1, 128), F32),
            pltpu.VMEM((n_tm, 1, 128), F32),
            dma((2, CHUNKS)),
            dma((max(rounds, 1), CHUNKS)),
            dma((max(rounds, 1), CHUNKS)),
            dma((n_path,)),
            dma((n_path,)),
            dma((n_tm,)),
            dma((n_tm,)),
        ],
        compiler_params=pltpu.CompilerParams(collective_id=0, has_side_effects=True),
    )(
        fx_vol,
        fx_corr,
        hazard_scale,
        counterparty[None],
        currency[None],
        maturity[None],
        notional[None],
        strike[None],
        shock_rate,
        shock_fx,
    )
    return (profile, cva.reshape(ncp))


def solution(mesh):
    return jax.shard_map(
        per_device,
        mesh=mesh,
        in_specs=(P("tm", "path"), P(None, "tm", "path"), P(), P(), P(), P(), P(), P(), P(), P()),
        out_specs=(P("tm", None), P()),
        check_vma=False,
    )
```
